256 devices in a mesh: gx: 8 (over x, z_lo), gy: 8 (over z_hi, core), gz: 4 (over y).
Axes of the slice: x: 4, y: 4, z: 8 (z_hi: 4, z_lo: 2; z = z_hi * 2 + z_lo), core: 2. Of those that a mesh axis runs over, the one named last changes fastest.
Arguments:
- partials: float32 [32, 128, 128, 512], P('gx', None, 'gy', 'gz'), may hold values from -40 to 40
- code_bits: int32 [32, 128], replicated, may hold values from 0 to 1
- group_map: int32 [32], replicated, may hold values from 0 to 31, each once
- velocity: float32 [128, 128, 512], P('gx', 'gy', 'gz'), may hold values from 1.5 to 4.5
Outputs:
- gradient: float32 [128, 128, 512], P('gx', 'gy', 'gz')
- new_model: float32 [128, 128, 512], P('gx', 'gy', 'gz')
The draws below stay inside these ranges and needn't reach their ends.
Inputs may be any that keep to these rules, and one draw needn't show every extreme that they name: `group_map`: every group of 0 to 31 stands in exactly one slot.
All inputs are finite; a program needn't handle non-finite values.
Results may differ from the reference program's by a relative error of at most 0.0001.
Values sent between devices are 32-bit elements; how exact they have to be, the bound alone decides.
A program may use at most 64 MiB of HBM per device.

```python
import jax
import jax.numpy as jnp
from jax import lax

G = 32
ITERS = 3
NX = 128
NY = 128
NZ = 512


def draw_partials(key, part):
    first_key = jax.random.fold_in(jax.random.fold_in(key, 17), 0)
    rough = jnp.clip(jax.random.normal(first_key, (G, NX, NY, NZ), jnp.float32), -6.0, 6.0)
    return rough


def set_ends(result, rng, smallest, top_value):
    longest = result.shape.index(max(result.shape))
    spots = []
    for shift in (0, 1):
        where = [jax.random.randint(jax.random.fold_in(rng, axis), (), 0, length) for axis, length in enumerate(result.shape)]
        where[longest] = (where[longest] + shift) % result.shape[longest]
        spots.append(tuple(where))
    return result.at[spots[0]].set(smallest).at[spots[1]].set(top_value)


def block_scale(key, dims, pieces, low, top_value):
    def one(axis_at, parts):
        draws = jax.random.uniform(jax.random.fold_in(jax.random.fold_in(key, 6), axis_at), (parts,), jnp.float32, low / len(pieces), top_value / len(pieces))
        return jnp.repeat(jnp.exp(draws), dims[axis_at] // parts).reshape((-1,) + (1,) * (len(dims) - axis_at - 1))

    loudness = one(*pieces[0])
    for cut in pieces[1:]:
        loudness = loudness * one(*cut)
    return loudness


def setup_inputs(seed: int = 0) -> dict:
    arg_keys = jax.random.split(jax.random.key(seed), 5)
    return {
        "partials": draw_partials(jax.random.fold_in(arg_keys[4], 71), 0),
        "code_bits": set_ends(jax.random.randint(arg_keys[1], (G, NX), 0, 2), jax.random.fold_in(arg_keys[1], 1), 0, 1).astype(jnp.int32),
        "group_map": jax.random.permutation(arg_keys[2], G).astype(jnp.int32),
        "velocity": jnp.clip(1.5 + 3.0 * jax.random.uniform(arg_keys[3], (NX, NY, NZ), jnp.float32) ** block_scale(arg_keys[3], (NX, NY, NZ), ((0, 8), (1, 8), (2, 4)), -0.2, 0.2), 1.5, 4.5),
    }


step_length = 0.5
tv_weight = 0.2
dual_step = 0.28
primal_step = 0.28

def forward_diff(field):
    zeros_x = jnp.zeros((1,) + field.shape[1:], jnp.float32)
    zeros_y = jnp.zeros((field.shape[0], 1, field.shape[2]), jnp.float32)
    zeros_z = jnp.zeros(field.shape[:2] + (1,), jnp.float32)
    diff_x = jnp.concatenate([field[1:] - field[:-1], zeros_x], 0)
    diff_y = jnp.concatenate([field[:, 1:] - field[:, :-1], zeros_y], 1)
    diff_z = jnp.concatenate([field[:, :, 1:] - field[:, :, :-1], zeros_z], 2)
    return jnp.stack([diff_x, diff_y, diff_z])

def divergence(dual_field):
    left_x = jnp.pad(dual_field[0][:-1], ((1, 0), (0, 0), (0, 0)))
    left_y = jnp.pad(dual_field[1][:, :-1], ((0, 0), (1, 0), (0, 0)))
    left_z = jnp.pad(dual_field[2][:, :, :-1], ((0, 0), (0, 0), (1, 0)))
    return dual_field[0] - left_x + (dual_field[1] - left_y) + (dual_field[2] - left_z)

def reference(partials, code_bits, group_map, velocity):
    sign_table = 2.0 * code_bits[group_map].astype(jnp.float32) - 1.0

    def accumulate(index, acc):
        return acc + sign_table[index][:, None, None] * partials[index]
    gradient = lax.fori_loop(0, partials.shape[0], accumulate, jnp.zeros(velocity.shape, jnp.float32))
    mean_square = jnp.sum(gradient * gradient) / gradient.size
    step_scale = step_length / jnp.sqrt(mean_square + 1.0)
    target = velocity - step_scale * gradient
    current = target
    extra = target
    dual_field = jnp.zeros((3,) + target.shape, jnp.float32)
    for iteration in range(ITERS):
        dual_field = dual_field + dual_step * forward_diff(extra)
        magnitude = jnp.sqrt(lax.optimization_barrier(jnp.sum(dual_field * dual_field, axis=0)))
        dual_field = dual_field / jnp.maximum(1.0, magnitude / tv_weight)[None]
        updated = (current + primal_step * divergence(dual_field) + primal_step * target) / (1.0 + primal_step)
        extra = 2.0 * updated - current
        current = updated
    return (gradient, current)
```

```python
import functools

import jax
import jax.numpy as jnp
from jax import lax
from jax.experimental import pallas as pl
from jax.experimental.pallas import tpu as pltpu
from jax.sharding import PartitionSpec as P

ITERS = 3
HALO = 3
STEP_LENGTH = 0.5
TV_WEIGHT = 0.2
DUAL_STEP = 0.28
PRIMAL_STEP = 0.28
MESH = pl.DeviceIdType.MESH

STREAMS = ((0, 5), (5, 10), (10, 16))
ORDERS = ((0, 1, 2), (1, 2, 0), (2, 0, 1))
HIGH = 5
LOW = 6


def flipped(x, zl, bits):
    bz, bp, bq = bits
    if bz:
        zl = 1 - zl
    if bp:
        x = x + 1 - 2 * (x % 2)
    if bq:
        x = 3 - x
    return x * 2 + zl


def cube_bits(order, idx):
    bits = [0, 0, 0]
    for place, dim in enumerate(order):
        bits[dim] = (idx >> (2 - place)) & 1
    return tuple(bits)


def comm_kernel(
    cells,
    partials, code_bits, group_map, velocity,
    t_out, eh_out, el_out, g_out,
    pin, w, r, xg, xv, packs, landed, ss, a1, a2, bits_s, map_s,
    load_sem, small_sem, rs_send, rs_recv, ar_send, ar_recv,
    h1_send, h1_recv, h2_send, h2_recv,
):
    gx, gy, gz = lax.axis_index("gx"), lax.axis_index("gy"), lax.axis_index("gz")
    x, zl = gx // 2, gx % 2
    zh, core = gy // 2, gy % 2
    z = zh * 2 + zl
    slots = partials.shape[0]
    rows = w.shape[1]

    bits_copy = pltpu.make_async_copy(code_bits, bits_s, small_sem.at[0])
    map_copy = pltpu.make_async_copy(group_map, map_s, small_sem.at[1])
    vel_copy = pltpu.make_async_copy(velocity, xv.at[HALO:HALO + rows, 8:24], small_sem.at[2])
    map_copy.start()
    bits_copy.start()
    loads = {}
    for first in (6, 4, 2, 0):
        for p, (r0, r1) in enumerate(STREAMS):
            for idx in (first + 1, first):
                dest = flipped(x, zl, cube_bits(ORDERS[p], idx))
                span = pl.ds(dest * rows + r0, r1 - r0)
                loads[idx, p] = pltpu.make_async_copy(
                    partials.at[:, span], pin.at[:, span], load_sem.at[p * 8 + idx]
                )
                loads[idx, p].start()
    vel_copy.start()

    flat = [
        (((x + rx) % 4) * 2 + zl, gy, (gz + ry) % 4)
        for rx in range(4) for ry in range(4) if rx or ry
    ]
    tall = []
    for rz in range(8):
        for rc in range(2):
            if rz or rc:
                zz = (z + rz) % 8
                tall.append((x * 2 + zz % 2, (zz // 2) * 2 + (core + rc) % 2, gz))
    gx_up, gx_down = (gx + 1) % 8, (gx + 7) % 8
    gy_up, gy_down = (gy + 1) % 8, (gy + 7) % 8
    diagonal = (gx + 7 + 2 * zl) % 8
    slanted = [(diagonal, gy, gz), (diagonal, gy_up, gz), (diagonal, gy_down, gz)]
    barrier = pltpu.get_barrier_semaphore()
    greeted = flat + tall + slanted
    for peer in greeted:
        pl.semaphore_signal(barrier, inc=1, device_id=peer, device_id_type=MESH)

    def weigh(idx, p):
        r0, r1 = STREAMS[p]
        dest = flipped(x, zl, cube_bits(ORDERS[p], idx))
        loads[idx, p].wait()
        for n in range(r0, r1):
            at = dest * rows + n
            total = None
            for i in range(slots):
                sign = 2.0 * bits_s[map_s[gx * slots + i], at].astype(jnp.float32) - 1.0
                term = sign * pin[i, at]
                total = term if total is None else total + term
            w[idx, n] = total

    def rs_copy(p, hop, src, dst):
        r0, r1 = STREAMS[p]
        place = (0, 0, 1, 1, 2)[hop]
        step = [0, 0, 0]
        step[ORDERS[p][place]] = 1
        return pltpu.make_async_remote_copy(
            src_ref=w.at[src, r0:r1],
            dst_ref=r.at[dst, r0:r1],
            send_sem=rs_send.at[p * 5 + hop],
            recv_sem=rs_recv.at[p * 5 + hop],
            device_id=(flipped(x, zl, step), gy, gz),
            device_id_type=MESH,
        )

    rs = {}
    for p in range(3):
        rs[p, 0] = rs_copy(p, 0, slice(6, 8), slice(2, 4))
        rs[p, 1] = rs_copy(p, 1, slice(4, 6), slice(0, 2))
        rs[p, 2] = rs_copy(p, 2, slice(3, 4), slice(5, 6))
        rs[p, 3] = rs_copy(p, 3, slice(2, 3), slice(4, 5))
        rs[p, 4] = rs_copy(p, 4, slice(1, 2), slice(6, 7))

    map_copy.wait()
    bits_copy.wait()
    for p in range(3):
        weigh(7, p)
        weigh(6, p)
        if p == 0:
            pl.semaphore_wait(barrier, len(greeted))
        rs[p, 0].start()
    for p in range(3):
        weigh(5, p)
        weigh(4, p)
        rs[p, 1].start()
    for p in range(3):
        weigh(3, p)
        weigh(2, p)
    for p in range(3):
        weigh(1, p)
        weigh(0, p)

    def gather_in(p, k, source):
        r0, r1 = STREAMS[p]
        w[k, r0:r1] = w[k, r0:r1] + r[source, r0:r1]

    for p in range(3):
        rs[p, 0].wait_recv()
        gather_in(p, 3, 3)
        rs[p, 2].start()
        gather_in(p, 2, 2)
        rs[p, 3].start()
    for p in range(3):
        rs[p, 1].wait_recv()
        gather_in(p, 1, 1)
        gather_in(p, 0, 0)
    for p in range(3):
        rs[p, 2].wait_recv()
        gather_in(p, 1, 5)
        rs[p, 4].start()

    def halo_copies(block, which):
        down, up = slice(HALO, 2 * HALO), slice(rows, rows + HALO)
        whole, below, above = slice(HALO, HALO + rows), slice(0, HALO), slice(HALO + rows, 2 * HALO + rows)
        first, last, both, under, over = slice(8, 16), slice(16, 24), slice(8, 24), slice(0, 8), slice(24, 32)
        moves = [
            ((gx_up, gy, gz), (up, both), (below, both)),
            ((gx_down, gy, gz), (down, both), (above, both)),
            ((gx, gy_up, gz), (whole, last), (whole, under)),
            ((gx, gy_down, gz), (whole, first), (whole, over)),
            ((gx_up, gy_up, gz), (up, last), (below, under)),
            ((gx_up, gy_down, gz), (up, first), (below, over)),
            ((gx_down, gy_up, gz), (down, last), (above, under)),
            ((gx_down, gy_down, gz), (down, first), (above, over)),
        ]
        return [
            pltpu.make_async_remote_copy(
                src_ref=block.at[src[0], src[1]],
                dst_ref=block.at[dst[0], dst[1]],
                send_sem=h1_send.at[which * 8 + n],
                recv_sem=h1_recv.at[which * 8 + n],
                device_id=peer,
                device_id_type=MESH,
            )
            for n, (peer, src, dst) in enumerate(moves)
        ]

    v_halo = halo_copies(xv, 0)
    g_halo = halo_copies(xg, 1)
    vel_copy.wait()
    for copy in v_halo:
        copy.start()

    square = jnp.zeros((8, 128), jnp.float32)
    for p, (r0, r1) in enumerate(STREAMS):
        rs[p, 3].wait_recv()
        gather_in(p, 0, 4)
    for p, (r0, r1) in enumerate(STREAMS):
        rs[p, 4].wait_recv()
        for n in range(r0, r1):
            value = w[0, n] + r[6, n]
            xg[HALO + n, 8:24] = value
            g_out[n] = value
            value = value * value
            square = square + (value[:8] + value[8:])
    ss[0] = square

    def reduce_copies(src, dst, base, peers):
        return [
            pltpu.make_async_remote_copy(
                src_ref=src,
                dst_ref=dst.at[n],
                send_sem=ar_send.at[base + n],
                recv_sem=ar_recv.at[base + n],
                device_id=peer,
                device_id_type=MESH,
            )
            for n, peer in enumerate(peers)
        ]

    ar1 = reduce_copies(ss.at[0], a1, 0, flat)
    ar2 = reduce_copies(ss.at[1], a2, 15, tall)
    for copy in ar1:
        copy.start()
    for copy in g_halo:
        copy.start()

    lane = lax.broadcasted_iota(jnp.int32, (24, 128), 1)
    low_half = lax.broadcasted_iota(jnp.int32, (8, 128), 0) < 4

    def ring_row(block, n):
        beyond = jnp.where(low_half, block[n, 24:32], block[n, 0:8])
        return jnp.concatenate([block[n, 8:24], beyond], 0)

    def pack(block, which):
        def one(n, carry):
            high, low = carry
            row = ring_row(block, n)
            at = lane - HIGH * n
            high = jnp.where((at >= 0) & (at < HIGH), pltpu.roll(row, HIGH * n + 2, 1), high)
            at = lane - LOW * (n - 1)
            low = jnp.where((at >= 0) & (at < LOW), pltpu.roll(row, (LOW * n + 125) % 128, 1), low)
            return high, low

        zero = jnp.zeros((24, 128), jnp.float32)
        high, low = lax.fori_loop(0, rows + 2 * HALO, one, (zero, zero))
        packs[2 * which] = high
        packs[2 * which + 1] = low

    def pack_copies(which):
        peers = [(gx, gy, (gz + 3) % 4), (gx, gy, (gz + 1) % 4)]
        return [
            pltpu.make_async_remote_copy(
                src_ref=packs.at[2 * which + n],
                dst_ref=landed.at[2 * which + n],
                send_sem=h2_send.at[2 * which + n],
                recv_sem=h2_recv.at[2 * which + n],
                device_id=peer,
                device_id_type=MESH,
            )
            for n, peer in enumerate(peers)
        ]

    v_pack, g_pack = pack_copies(0), pack_copies(1)
    for copy in v_halo:
        copy.wait_recv()
    pack(xv, 0)
    for copy in v_pack:
        copy.start()

    for copy in ar1:
        copy.wait_recv()
    total = ss[0]
    for n in range(15):
        total = total + a1[n]
    ss[1] = total
    for copy in ar2:
        copy.start()

    for copy in g_halo:
        copy.wait_recv()
    pack(xg, 1)
    for copy in g_pack:
        copy.start()

    for copy in ar2:
        copy.wait_recv()
    total = ss[1]
    for n in range(15):
        total = total + a2[n]
    mean_square = jnp.sum(total, keepdims=True) * (1.0 / cells)
    scale = STEP_LENGTH * lax.rsqrt(mean_square + 1.0)

    def target_row(n, carry):
        t_out[n] = ring_row(xv, n) - scale * ring_row(xg, n)
        return carry

    lax.fori_loop(0, rows + 2 * HALO, target_row, 0)
    for copy in v_pack + g_pack:
        copy.wait_recv()
    eh_out[0] = packs[0] - scale * packs[2]
    el_out[0] = packs[1] - scale * packs[3]
    eh_out[1] = landed[0] - scale * landed[2]
    el_out[1] = landed[1] - scale * landed[3]

    for p in range(3):
        for hop in range(5):
            rs[p, hop].wait_send()
    for copy in v_halo + g_halo + v_pack + g_pack + ar1 + ar2:
        copy.wait_send()


def tv_kernel(sizes, t_in, eh_in, el_in, g_in, g_out, u_out, cur, bar, dx, dy, dz):
    nx, ny, nz = sizes
    gx, gy, gz = lax.axis_index("gx"), lax.axis_index("gy"), lax.axis_index("gz")
    rows = g_in.shape[0]
    lanes = 128
    shape = (24, 128)
    lane = lax.broadcasted_iota(jnp.int32, shape, 1)
    ring = lax.broadcasted_iota(jnp.int32, shape, 0)

    def steps(position, count):
        inside = (position >= 0) & (position < count - 1)
        return jnp.where(inside, jnp.float32(DUAL_STEP), jnp.float32(0.0))

    step_y = steps(gy * 16 + jnp.where(ring < 20, ring, ring - 24), ny)
    step_z = steps(gz * lanes + lane, nz)
    step_x = [steps(gx * rows + n - HALO, nx) for n in range(rows + 2 * HALO)]

    g_out[...] = g_in[...]

    def shrink(a, b, c):
        norm = a * a + b * b + c * c
        limit = TV_WEIGHT * TV_WEIGHT
        return jnp.where(norm > limit, TV_WEIGHT * lax.rsqrt(norm), 1.0)

    def up(field, axis, by=1):
        return pltpu.roll(field, field.shape[axis] - by, axis)

    def down(field, axis, by=1):
        return pltpu.roll(field, by, axis)

    def primal(current, spread, target_part):
        return (current + PRIMAL_STEP * spread + target_part) * (1.0 / (1.0 + PRIMAL_STEP))

    class Edge:
        def __init__(self, own, other, width, first_row, first_plane, mine):
            plane = lane % width
            self.width = width
            self.target = jnp.where(mine(plane), own, other)
            self.tpart = PRIMAL_STEP * self.target
            self.current = self.bar = self.target
            self.step_x = steps(gx * rows + first_row + lane // width, nx)
            self.step_z = steps(gz * lanes + first_plane + plane, nz)
            self.dual = None

        def ascend(self):
            b = self.bar
            a = self.step_x * (up(b, 1, self.width) - b)
            c = step_y * (up(b, 0) - b)
            d = self.step_z * (up(b, 1) - b)
            if self.dual is not None:
                a, c, d = self.dual[0] + a, self.dual[1] + c, self.dual[2] + d
            f = shrink(a, c, d)
            self.dual = (a * f, c * f, d * f)

        def descend(self):
            a, c, d = self.dual
            spread = (a - down(a, 1, self.width)) + (c - down(c, 0)) + (d - down(d, 1))
            new = primal(self.current, spread, self.tpart)
            self.bar = 2.0 * new - self.current
            self.current = new

    high = Edge(eh_in[0], eh_in[1], HIGH, -HALO, lanes - 2, lambda k: k < 2)
    low = Edge(el_in[0], el_in[1], LOW, 1 - HALO, -3, lambda k: k >= 3)

    last = lane == lanes - 1
    head = lane == 0
    for it in range(ITERS):
        final = it == ITERS - 1
        source = t_in if it == 0 else bar
        present = t_in if it == 0 else cur
        above = high.bar
        low.ascend()
        below = low.dual[2]
        if not final:
            low.descend()
            high.ascend()
            high.descend()
        stop = rows + 2 * HALO - 1 - it
        previous_dx = None
        here = source[it]
        for n in range(it, stop):
            after = source[n + 1]
            beyond = pltpu.roll(above, (lanes - 1 - (HIGH * n + 2)) % lanes, 1)
            a = step_x[n] * (after - here)
            b = step_y * (up(here, 0) - here)
            c = step_z * (jnp.where(last, beyond, up(here, 1)) - here)
            if it:
                a, b, c = dx[n] + a, dy[n] + b, dz[n] + c
            f = shrink(a, b, c)
            a, b, c = a * f, b * f, c * f
            if not final:
                dx[n], dy[n], dz[n] = a, b, c
            if n > it:
                under = pltpu.roll(below, (lanes - (LOW * (n - 1) + 2)) % lanes, 1)
                spread = (a - previous_dx) + (b - down(b, 0)) + (c - jnp.where(head, under, down(c, 1)))
                now = present[n]
                new = primal(now, spread, PRIMAL_STEP * t_in[n])
                if final:
                    u_out[n - HALO] = new[:16]
                else:
                    bar[n] = 2.0 * new - now
                    cur[n] = new
            previous_dx = a
            here = after


def shards(partials, code_bits, group_map, velocity):
    slots, nx, block_y, block_z = partials.shape
    block_x = velocity.shape[0]
    sizes = (
        block_x * lax.axis_size("gx"),
        block_y * lax.axis_size("gy"),
        block_z * lax.axis_size("gz"),
    )
    wide = block_x + 2 * HALO
    f32 = functools.partial(pltpu.VMEM, dtype=jnp.float32)
    dma = pltpu.SemaphoreType.DMA
    hbm = pl.BlockSpec(memory_space=pltpu.HBM)
    vmem = pl.BlockSpec(memory_space=pltpu.VMEM)
    packed = jax.ShapeDtypeStruct((2, 24, 128), jnp.float32)
    block = jax.ShapeDtypeStruct(velocity.shape, jnp.float32)
    target, high, low, gradient = pl.pallas_call(
        functools.partial(comm_kernel, sizes[0] * sizes[1] * sizes[2]),
        out_shape=(
            jax.ShapeDtypeStruct((wide, 24, 128), jnp.float32), packed, packed, block,
        ),
        in_specs=[hbm] * 4,
        out_specs=(vmem,) * 4,
        scratch_shapes=[
            f32(partials.shape),
            f32((8, block_x, 16, 128)),
            f32((7, block_x, 16, 128)),
            f32((wide, 32, 128)),
            f32((wide, 32, 128)),
            f32((4, 24, 128)),
            f32((4, 24, 128)),
            f32((2, 8, 128)),
            f32((15, 8, 128)),
            f32((15, 8, 128)),
            pltpu.SMEM(code_bits.shape, jnp.int32),
            pltpu.SMEM(group_map.shape, jnp.int32),
            dma((24,)), dma((3,)), dma((15,)), dma((15,)), dma((30,)), dma((30,)),
            dma((16,)), dma((16,)), dma((4,)), dma((4,)),
        ],
        compiler_params=pltpu.CompilerParams(
            collective_id=0, has_side_effects=True, vmem_limit_bytes=48 * 1024 * 1024
        ),
        name="decode_exchange",
    )(partials, code_bits, group_map, velocity)
    field = f32((wide, 24, 128))
    return pl.pallas_call(
        functools.partial(tv_kernel, sizes),
        out_shape=(block, block),
        in_specs=[vmem] * 4,
        out_specs=(vmem, vmem),
        scratch_shapes=[field] * 5,
        name="tv_steps",
    )(target, high, low, gradient)


def solution(mesh):
    split = P("gx", "gy", "gz")
    return jax.shard_map(
        shards,
        mesh=mesh,
        in_specs=(P("gx", None, "gy", "gz"), P(), P(), split),
        out_specs=(split, split),
        check_vma=False,
    )
```

```python
import functools

import jax
import jax.numpy as jnp
from jax import lax
from jax.experimental import pallas as pl
from jax.experimental.pallas import tpu as pltpu
from jax.sharding import PartitionSpec as P

ITERS = 3
HALO = 3
STEP_LENGTH = 0.5
TV_WEIGHT = 0.2
DUAL_STEP = 0.28
PRIMAL_STEP = 0.28
MESH = pl.DeviceIdType.MESH

STREAMS = ((0, 5), (5, 10), (10, 16))
ORDERS = ((0, 1, 2), (1, 2, 0), (2, 0, 1))
HIGH = 5
LOW = 6


def flipped(x, zl, bits):
    bz, bp, bq = bits
    if bz:
        zl = 1 - zl
    if bp:
        x = x + 1 - 2 * (x % 2)
    if bq:
        x = 3 - x
    return x * 2 + zl


def cube_bits(order, idx):
    bits = [0, 0, 0]
    for place, dim in enumerate(order):
        bits[dim] = (idx >> (2 - place)) & 1
    return tuple(bits)


def comm_kernel(
    cells,
    partials, code_bits, group_map, velocity,
    t_out, eh_out, el_out, g_out,
    pin, w, r, xg, xv, packs, landed, ss, a1, a2, bits_s, map_s,
    load_sem, small_sem, rs_send, rs_recv, ar_send, ar_recv,
    h1_send, h1_recv, h2_send, h2_recv,
):
    gx, gy, gz = lax.axis_index("gx"), lax.axis_index("gy"), lax.axis_index("gz")
    x, zl = gx // 2, gx % 2
    zh, core = gy // 2, gy % 2
    z = zh * 2 + zl
    slots = partials.shape[0]
    rows = w.shape[1]

    bits_copy = pltpu.make_async_copy(code_bits, bits_s, small_sem.at[0])
    map_copy = pltpu.make_async_copy(group_map, map_s, small_sem.at[1])
    vel_copy = pltpu.make_async_copy(velocity, xv.at[HALO:HALO + rows, 8:24], small_sem.at[2])
    map_copy.start()
    bits_copy.start()
    loads = {}
    for first in (6, 4, 2, 0):
        for p, (r0, r1) in enumerate(STREAMS):
            for idx in (first + 1, first):
                dest = flipped(x, zl, cube_bits(ORDERS[p], idx))
                span = pl.ds(dest * rows + r0, r1 - r0)
                loads[idx, p] = pltpu.make_async_copy(
                    partials.at[:, span], pin.at[:, span], load_sem.at[p * 8 + idx]
                )
                loads[idx, p].start()
    vel_copy.start()

    flat = [
        (((x + rx) % 4) * 2 + zl, gy, (gz + ry) % 4)
        for rx in range(4) for ry in range(4) if rx or ry
    ]
    tall = []
    for rz in range(8):
        for rc in range(2):
            if rz or rc:
                zz = (z + rz) % 8
                tall.append((x * 2 + zz % 2, (zz // 2) * 2 + (core + rc) % 2, gz))
    gx_up, gx_down = (gx + 1) % 8, (gx + 7) % 8
    gy_up, gy_down = (gy + 1) % 8, (gy + 7) % 8
    diagonal = (gx + 7 + 2 * zl) % 8
    slanted = [(diagonal, gy, gz), (diagonal, gy_up, gz), (diagonal, gy_down, gz)]
    barrier = pltpu.get_barrier_semaphore()
    greeted = flat + tall + slanted
    for peer in greeted:
        pl.semaphore_signal(barrier, inc=1, device_id=peer, device_id_type=MESH)

    def weigh(idx, p):
        r0, r1 = STREAMS[p]
        dest = flipped(x, zl, cube_bits(ORDERS[p], idx))
        loads[idx, p].wait()
        for n in range(r0, r1):
            at = dest * rows + n
            total = None
            for i in range(slots):
                sign = 2.0 * bits_s[map_s[gx * slots + i], at].astype(jnp.float32) - 1.0
                term = sign * pin[i, at]
                total = term if total is None else total + term
            w[idx, n] = total

    def rs_copy(p, hop, src, dst):
        r0, r1 = STREAMS[p]
        place = (0, 0, 1, 1, 2)[hop]
        step = [0, 0, 0]
        step[ORDERS[p][place]] = 1
        return pltpu.make_async_remote_copy(
            src_ref=w.at[src, r0:r1],
            dst_ref=r.at[dst, r0:r1],
            send_sem=rs_send.at[p * 5 + hop],
            recv_sem=rs_recv.at[p * 5 + hop],
            device_id=(flipped(x, zl, step), gy, gz),
            device_id_type=MESH,
        )

    rs = {}
    for p in range(3):
        rs[p, 0] = rs_copy(p, 0, slice(6, 8), slice(2, 4))
        rs[p, 1] = rs_copy(p, 1, slice(4, 6), slice(0, 2))
        rs[p, 2] = rs_copy(p, 2, slice(3, 4), slice(5, 6))
        rs[p, 3] = rs_copy(p, 3, slice(2, 3), slice(4, 5))
        rs[p, 4] = rs_copy(p, 4, slice(1, 2), slice(6, 7))

    with jax.named_scope("load_bits"):
        map_copy.wait()
        bits_copy.wait()
    with jax.named_scope("weigh_first"):
        weigh(7, 0)
        weigh(6, 0)
    with jax.named_scope("entry_barrier"):
        pl.semaphore_wait(barrier, len(greeted))
    with jax.named_scope("weigh_sent"):
        rs[0, 0].start()
        for p in (1, 2):
            weigh(7, p)
            weigh(6, p)
            rs[p, 0].start()
        for p in range(3):
            weigh(5, p)
            weigh(4, p)
            rs[p, 1].start()
    with jax.named_scope("weigh_rest"):
        for p in range(3):
            weigh(3, p)
            weigh(2, p)
        for p in range(3):
            weigh(1, p)
            weigh(0, p)

    def gather_in(p, k, source):
        r0, r1 = STREAMS[p]
        w[k, r0:r1] = w[k, r0:r1] + r[source, r0:r1]

    for p in range(3):
        with jax.named_scope(f"hop1a#p={p}"):
            rs[p, 0].wait_recv()
            gather_in(p, 3, 3)
            rs[p, 2].start()
            gather_in(p, 2, 2)
            rs[p, 3].start()
    for p in range(3):
        with jax.named_scope(f"hop1b#p={p}"):
            rs[p, 1].wait_recv()
            gather_in(p, 1, 1)
            gather_in(p, 0, 0)
    for p in range(3):
        with jax.named_scope(f"hop2a#p={p}"):
            rs[p, 2].wait_recv()
            gather_in(p, 1, 5)
            rs[p, 4].start()

    def halo_copies(block, which):
        down, up = slice(HALO, 2 * HALO), slice(rows, rows + HALO)
        whole, below, above = slice(HALO, HALO + rows), slice(0, HALO), slice(HALO + rows, 2 * HALO + rows)
        first, last, both, under, over = slice(8, 16), slice(16, 24), slice(8, 24), slice(0, 8), slice(24, 32)
        moves = [
            ((gx_up, gy, gz), (up, both), (below, both)),
            ((gx_down, gy, gz), (down, both), (above, both)),
            ((gx, gy_up, gz), (whole, last), (whole, under)),
            ((gx, gy_down, gz), (whole, first), (whole, over)),
            ((gx_up, gy_up, gz), (up, last), (below, under)),
            ((gx_up, gy_down, gz), (up, first), (below, over)),
            ((gx_down, gy_up, gz), (down, last), (above, under)),
            ((gx_down, gy_down, gz), (down, first), (above, over)),
        ]
        return [
            pltpu.make_async_remote_copy(
                src_ref=block.at[src[0], src[1]],
                dst_ref=block.at[dst[0], dst[1]],
                send_sem=h1_send.at[which * 8 + n],
                recv_sem=h1_recv.at[which * 8 + n],
                device_id=peer,
                device_id_type=MESH,
            )
            for n, (peer, src, dst) in enumerate(moves)
        ]

    v_halo = halo_copies(xv, 0)
    g_halo = halo_copies(xg, 1)
    with jax.named_scope("velocity_halo"):
        vel_copy.wait()
        for copy in v_halo:
            copy.start()

    with jax.named_scope("hop2b"):
        for p in range(3):
            rs[p, 3].wait_recv()
            gather_in(p, 0, 4)
    square = jnp.zeros((8, 128), jnp.float32)
    with jax.named_scope("hop3"):
        for p, (r0, r1) in enumerate(STREAMS):
            rs[p, 4].wait_recv()
            for n in range(r0, r1):
                value = w[0, n] + r[6, n]
                xg[HALO + n, 8:24] = value
                g_out[n] = value
                value = value * value
                square = square + (value[:8] + value[8:])
        ss[0] = square

    def reduce_copies(src, dst, base, peers):
        return [
            pltpu.make_async_remote_copy(
                src_ref=src,
                dst_ref=dst.at[n],
                send_sem=ar_send.at[base + n],
                recv_sem=ar_recv.at[base + n],
                device_id=peer,
                device_id_type=MESH,
            )
            for n, peer in enumerate(peers)
        ]

    ar1 = reduce_copies(ss.at[0], a1, 0, flat)
    ar2 = reduce_copies(ss.at[1], a2, 15, tall)
    with jax.named_scope("send_squares"):
        for copy in ar1:
            copy.start()
        for copy in g_halo:
            copy.start()

    lane = lax.broadcasted_iota(jnp.int32, (24, 128), 1)
    low_half = lax.broadcasted_iota(jnp.int32, (8, 128), 0) < 4

    def ring_row(block, n):
        beyond = jnp.where(low_half, block[n, 24:32], block[n, 0:8])
        return jnp.concatenate([block[n, 8:24], beyond], 0)

    def pack(block, which):
        def one(n, carry):
            high, low = carry
            row = ring_row(block, n)
            at = lane - HIGH * n
            high = jnp.where((at >= 0) & (at < HIGH), pltpu.roll(row, HIGH * n + 2, 1), high)
            at = lane - LOW * (n - 1)
            low = jnp.where((at >= 0) & (at < LOW), pltpu.roll(row, (LOW * n + 125) % 128, 1), low)
            return high, low

        zero = jnp.zeros((24, 128), jnp.float32)
        high, low = lax.fori_loop(0, rows + 2 * HALO, one, (zero, zero))
        packs[2 * which] = high
        packs[2 * which + 1] = low

    def pack_copies(which):
        peers = [(gx, gy, (gz + 3) % 4), (gx, gy, (gz + 1) % 4)]
        return [
            pltpu.make_async_remote_copy(
                src_ref=packs.at[2 * which + n],
                dst_ref=landed.at[2 * which + n],
                send_sem=h2_send.at[2 * which + n],
                recv_sem=h2_recv.at[2 * which + n],
                device_id=peer,
                device_id_type=MESH,
            )
            for n, peer in enumerate(peers)
        ]

    v_pack, g_pack = pack_copies(0), pack_copies(1)
    with jax.named_scope("wait_v_halo"):
        for copy in v_halo:
            copy.wait_recv()
    with jax.named_scope("pack_v"):
        pack(xv, 0)
        for copy in v_pack:
            copy.start()

    with jax.named_scope("wait_squares1"):
        for copy in ar1:
            copy.wait_recv()
        total = ss[0]
        for n in range(15):
            total = total + a1[n]
        ss[1] = total
        for copy in ar2:
            copy.start()

    with jax.named_scope("wait_g_halo"):
        for copy in g_halo:
            copy.wait_recv()
    with jax.named_scope("pack_g"):
        pack(xg, 1)
        for copy in g_pack:
            copy.start()

    with jax.named_scope("wait_squares2"):
        for copy in ar2:
            copy.wait_recv()
    total = ss[1]
    for n in range(15):
        total = total + a2[n]
    mean_square = jnp.sum(total, keepdims=True) * (1.0 / cells)
    scale = STEP_LENGTH * lax.rsqrt(mean_square + 1.0)

    def target_row(n, carry):
        t_out[n] = ring_row(xv, n) - scale * ring_row(xg, n)
        return carry

    with jax.named_scope("target"):
        lax.fori_loop(0, rows + 2 * HALO, target_row, 0)
    with jax.named_scope("wait_packs"):
        for copy in v_pack + g_pack:
            copy.wait_recv()
        eh_out[0] = packs[0] - scale * packs[2]
        el_out[0] = packs[1] - scale * packs[3]
        eh_out[1] = landed[0] - scale * landed[2]
        el_out[1] = landed[1] - scale * landed[3]

    with jax.named_scope("drain"):
        for p in range(3):
            for hop in range(5):
                rs[p, hop].wait_send()
        for copy in v_halo + g_halo + v_pack + g_pack + ar1 + ar2:
            copy.wait_send()


def tv_kernel(sizes, t_in, eh_in, el_in, g_in, g_out, u_hbm, cur, bar, dx, dy, dz, u_out, out_sem):
    nx, ny, nz = sizes
    gx, gy, gz = lax.axis_index("gx"), lax.axis_index("gy"), lax.axis_index("gz")
    rows = g_in.shape[0]
    lanes = 128
    shape = (24, 128)
    lane = lax.broadcasted_iota(jnp.int32, shape, 1)
    ring = lax.broadcasted_iota(jnp.int32, shape, 0)

    def steps(position, count):
        inside = (position >= 0) & (position < count - 1)
        return jnp.where(inside, jnp.float32(DUAL_STEP), jnp.float32(0.0))

    step_y = steps(gy * 16 + jnp.where(ring < 20, ring, ring - 24), ny)
    step_z = steps(gz * lanes + lane, nz)
    step_x = [steps(gx * rows + n - HALO, nx) for n in range(rows + 2 * HALO)]

    g_copy = pltpu.make_async_copy(g_in, g_out, out_sem.at[0])
    g_copy.start()

    def shrink(a, b, c):
        norm = a * a + b * b + c * c
        limit = TV_WEIGHT * TV_WEIGHT
        return jnp.where(norm > limit, TV_WEIGHT * lax.rsqrt(norm), 1.0)

    def up(field, axis, by=1):
        return pltpu.roll(field, field.shape[axis] - by, axis)

    def down(field, axis, by=1):
        return pltpu.roll(field, by, axis)

    def primal(current, spread, target_part):
        return (current + PRIMAL_STEP * spread + target_part) * (1.0 / (1.0 + PRIMAL_STEP))

    class Edge:
        def __init__(self, own, other, width, first_row, first_plane, mine):
            plane = lane % width
            self.width = width
            self.target = jnp.where(mine(plane), own, other)
            self.tpart = PRIMAL_STEP * self.target
            self.current = self.bar = self.target
            self.step_x = steps(gx * rows + first_row + lane // width, nx)
            self.step_z = steps(gz * lanes + first_plane + plane, nz)
            self.dual = None

        def ascend(self):
            b = self.bar
            a = self.step_x * (up(b, 1, self.width) - b)
            c = step_y * (up(b, 0) - b)
            d = self.step_z * (up(b, 1) - b)
            if self.dual is not None:
                a, c, d = self.dual[0] + a, self.dual[1] + c, self.dual[2] + d
            f = shrink(a, c, d)
            self.dual = (a * f, c * f, d * f)

        def descend(self):
            a, c, d = self.dual
            spread = (a - down(a, 1, self.width)) + (c - down(c, 0)) + (d - down(d, 1))
            new = primal(self.current, spread, self.tpart)
            self.bar = 2.0 * new - self.current
            self.current = new

    high = Edge(eh_in[0], eh_in[1], HIGH, -HALO, lanes - 2, lambda k: k < 2)
    low = Edge(el_in[0], el_in[1], LOW, 1 - HALO, -3, lambda k: k >= 3)

    last = lane == lanes - 1
    head = lane == 0
    for it in range(ITERS):
        final = it == ITERS - 1
        source = t_in if it == 0 else bar
        present = t_in if it == 0 else cur
        above = high.bar
        low.ascend()
        below = low.dual[2]
        if not final:
            low.descend()
            high.ascend()
            high.descend()
        stop = rows + 2 * HALO - 1 - it
        previous_dx = None
        here = source[it]
        for n in range(it, stop):
            after = source[n + 1]
            beyond = pltpu.roll(above, (lanes - 1 - (HIGH * n + 2)) % lanes, 1)
            a = step_x[n] * (after - here)
            b = step_y * (up(here, 0) - here)
            c = step_z * (jnp.where(last, beyond, up(here, 1)) - here)
            if it:
                a, b, c = dx[n] + a, dy[n] + b, dz[n] + c
            f = shrink(a, b, c)
            a, b, c = a * f, b * f, c * f
            if not final:
                dx[n], dy[n], dz[n] = a, b, c
            if n > it:
                under = pltpu.roll(below, (lanes - (LOW * (n - 1) + 2)) % lanes, 1)
                spread = (a - previous_dx) + (b - down(b, 0)) + (c - jnp.where(head, under, down(c, 1)))
                now = present[n]
                new = primal(now, spread, PRIMAL_STEP * t_in[n])
                if final:
                    u_out[n - HALO] = new[:16]
                else:
                    bar[n] = 2.0 * new - now
                    cur[n] = new
            previous_dx = a
            here = after

    u_copy = pltpu.make_async_copy(u_out, u_hbm, out_sem.at[1])
    u_copy.start()
    g_copy.wait()
    u_copy.wait()


def shards(partials, code_bits, group_map, velocity):
    slots, nx, block_y, block_z = partials.shape
    block_x = velocity.shape[0]
    sizes = (
        block_x * lax.axis_size("gx"),
        block_y * lax.axis_size("gy"),
        block_z * lax.axis_size("gz"),
    )
    wide = block_x + 2 * HALO
    f32 = functools.partial(pltpu.VMEM, dtype=jnp.float32)
    dma = pltpu.SemaphoreType.DMA
    hbm = pl.BlockSpec(memory_space=pltpu.HBM)
    vmem = pl.BlockSpec(memory_space=pltpu.VMEM)
    packed = f32((2, 24, 128))
    block = f32(velocity.shape)
    result = pltpu.HBM(velocity.shape, jnp.float32)
    target, high, low, gradient = pl.pallas_call(
        functools.partial(comm_kernel, sizes[0] * sizes[1] * sizes[2]),
        out_shape=(
            f32((wide, 24, 128)), packed, packed, block,
        ),
        in_specs=[hbm] * 4,
        out_specs=(vmem,) * 4,
        scratch_shapes=[
            f32(partials.shape),
            f32((8, block_x, 16, 128)),
            f32((7, block_x, 16, 128)),
            f32((wide, 32, 128)),
            f32((wide, 32, 128)),
            f32((4, 24, 128)),
            f32((4, 24, 128)),
            f32((2, 8, 128)),
            f32((15, 8, 128)),
            f32((15, 8, 128)),
            pltpu.SMEM(code_bits.shape, jnp.int32),
            pltpu.SMEM(group_map.shape, jnp.int32),
            dma((24,)), dma((3,)), dma((15,)), dma((15,)), dma((30,)), dma((30,)),
            dma((16,)), dma((16,)), dma((4,)), dma((4,)),
        ],
        compiler_params=pltpu.CompilerParams(
            collective_id=0, has_side_effects=True, vmem_limit_bytes=48 * 1024 * 1024
        ),
        name="decode_exchange",
    )(*(pltpu.with_memory_space_constraint(a, pltpu.HBM) for a in (partials, code_bits, group_map, velocity)))
    field = f32((wide, 24, 128))
    return pl.pallas_call(
        functools.partial(tv_kernel, sizes),
        out_shape=(result, result),
        in_specs=[vmem] * 4,
        out_specs=(hbm, hbm),
        scratch_shapes=[field] * 5 + [block, dma((2,))],
        compiler_params=pltpu.CompilerParams(vmem_limit_bytes=32 * 1024 * 1024),
        name="tv_steps",
    )(*(pltpu.with_memory_space_constraint(a, pltpu.VMEM) for a in (target, high, low, gradient)))


def solution(mesh):
    split = P("gx", "gy", "gz")
    return jax.shard_map(
        shards,
        mesh=mesh,
        in_specs=(P("gx", None, "gy", "gz"), P(), P(), split),
        out_specs=(split, split),
        check_vma=False,
    )
```

```python
import functools

import jax
import jax.numpy as jnp
from jax import lax
from jax.experimental import pallas as pl
from jax.experimental.pallas import tpu as pltpu
from jax.sharding import PartitionSpec as P

ITERS = 3
HALO = 3
STEP_LENGTH = 0.5
TV_WEIGHT = 0.2
DUAL_STEP = 0.28
PRIMAL_STEP = 0.28
MESH = pl.DeviceIdType.MESH

STREAMS = ((0, 5), (5, 10), (10, 16))
ORDERS = ((0, 1, 2), (1, 2, 0), (2, 0, 1))
HIGH = 5
LOW = 6


def flipped(x, zl, bits):
    bz, bp, bq = bits
    if bz:
        zl = 1 - zl
    if bp:
        x = x + 1 - 2 * (x % 2)
    if bq:
        x = 3 - x
    return x * 2 + zl


def cube_bits(order, idx):
    bits = [0, 0, 0]
    for place, dim in enumerate(order):
        bits[dim] = (idx >> (2 - place)) & 1
    return tuple(bits)


def comm_kernel(
    cells,
    partials, code_bits, group_map, velocity,
    t_out, eh_out, el_out, g_out,
    pin, w, r, vel, faces, sides, ends, packs, landed, ring_g, ss, a1, a2, bits_s, map_s,
    load_sem, small_sem, rs_send, rs_recv, ar_sem, halo_sem, pack_sem, met,
):
    gx, gy, gz = lax.axis_index("gx"), lax.axis_index("gy"), lax.axis_index("gz")
    x, zl = gx // 2, gx % 2
    zh, core = gy // 2, gy % 2
    z = zh * 2 + zl
    slots = partials.shape[0]
    rows = w.shape[1]
    wide = rows + 2 * HALO

    def along_x(step):
        return (((x + step + 4) % 4) * 2 + zl, gy, gz)

    def along_y(step):
        return (gx, gy, (gz + step + 4) % 4)

    def along_z(step):
        zz = (z + step + 8) % 8
        return (x * 2 + zz % 2, (zz // 2) * 2 + core, gz)

    def remote(src, dst, send_sem, recv_sem, peer):
        return pltpu.make_async_remote_copy(
            src_ref=src, dst_ref=dst, send_sem=send_sem, recv_sem=recv_sem,
            device_id=peer, device_id_type=MESH,
        )

    bits_copy = pltpu.make_async_copy(code_bits, bits_s, small_sem.at[0])
    map_copy = pltpu.make_async_copy(group_map, map_s, small_sem.at[1])
    vel_copy = pltpu.make_async_copy(velocity, vel, small_sem.at[2])
    map_copy.start()
    bits_copy.start()

    near = [along_x(1), along_x(-1), along_y(1), along_y(-1), along_z(1), along_z(-1)]
    near.append((gx, zh * 2 + 1 - core, gz))
    barrier = pltpu.get_barrier_semaphore()
    for peer in near:
        pl.semaphore_signal(barrier, inc=1, device_id=peer, device_id_type=MESH)

    def load_span(idx, p):
        r0, r1 = STREAMS[p]
        dest = flipped(x, zl, cube_bits(ORDERS[p], idx))
        return dest * rows + r0, r1 - r0

    for pair in (3, 2, 1, 0):
        for idx in (2 * pair + 1, 2 * pair):
            for p in range(3):
                start, count = load_span(idx, p)
                span = pl.ds(start, count)
                pltpu.make_async_copy(
                    partials.at[:, span], pin.at[:, span], load_sem.at[p * 4 + pair]
                ).start()
    vel_copy.start()

    def weigh(idx, p):
        start, count = load_span(idx, p)
        if idx % 2:
            both = pl.ds(0, 2 * count)
            pltpu.make_async_copy(
                partials.at[:, both], pin.at[:, both], load_sem.at[p * 4 + idx // 2]
            ).wait()
        for n in range(count):
            total = None
            for i in range(slots):
                sign = 2.0 * bits_s[map_s[gx * slots + i], start + n].astype(jnp.float32) - 1.0
                term = sign * pin[i, start + n]
                total = term if total is None else total + term
            w[idx, STREAMS[p][0] + n] = total

    sends = ((7, 3, 0), (6, 2, 0), (5, 1, 0), (4, 0, 0), (3, 5, 1), (2, 4, 1), (1, 6, 2))
    rs = {}
    for p, (r0, r1) in enumerate(STREAMS):
        for n, (src, dst, place) in enumerate(sends):
            step = [0, 0, 0]
            step[ORDERS[p][place]] = 1
            rs[p, src] = remote(
                w.at[src, r0:r1], r.at[dst, r0:r1], rs_send.at[0], rs_recv.at[p * 7 + n],
                (flipped(x, zl, step), gy, gz),
            )

    def meet(which, peers):
        for peer in peers:
            pl.semaphore_signal(met.at[which], inc=1, device_id=peer, device_id_type=MESH)

    with jax.named_scope("load_bits"):
        map_copy.wait()
        bits_copy.wait()
    with jax.named_scope("weigh_first"):
        weigh(7, 0)
    with jax.named_scope("entry_barrier"):
        pl.semaphore_wait(barrier, len(near))
    with jax.named_scope("weigh_sent"):
        rs[0, 7].start()
        for p in (1, 2):
            weigh(7, p)
            rs[p, 7].start()
        for idx in (6, 5):
            for p in range(3):
                weigh(idx, p)
                rs[p, idx].start()
    with jax.named_scope("weigh_rest"):
        meet(0, [along_y(1), along_y(-1), along_z(1), along_z(-1)])
        for idx in (3, 4, 2, 1, 0):
            for p in range(3):
                weigh(idx, p)

    low_half = lax.broadcasted_iota(jnp.int32, (8, 128), 0) < 4

    def fold_faces(block, which):
        for k in range(8):
            faces[which, 0, k] = jnp.where(low_half, pltpu.roll(block[k + 8, 8:16], 4, 0), block[k, 8:16])
            faces[which, 1, k] = jnp.where(low_half, block[k, 0:8], pltpu.roll(block[k + 8, 0:8], 4, 0))

    with jax.named_scope("meet_more"):
        vel_copy.wait()
        fold_faces(vel, 0)
        pl.semaphore_wait(met.at[0], 4)
        meet(1, [along_x(1), along_x(-1), along_z(2), along_z(-2)])

    def add_in(p, k, *sources):
        r0, r1 = STREAMS[p]
        for n in range(r0, r1):
            total = w[k, n]
            for source in sources:
                total = total + r[source, n]
            w[k, n] = total

    for p in range(3):
        with jax.named_scope(f"hop1a#p={p}"):
            rs[p, 7].wait_recv()
            add_in(p, 3, 3)
            rs[p, 3].start()
            rs[(p + 1) % 3, 4].start()
    for p in range(3):
        with jax.named_scope(f"hop1b#p={p}"):
            rs[p, 6].wait_recv()
            add_in(p, 2, 2)
            rs[p, 2].start()
    with jax.named_scope("meet_last"):
        pl.semaphore_wait(met.at[1], 4)
        meet(2, [along_x(1), along_x(-1)])
    for p in range(3):
        with jax.named_scope(f"hop2a#p={p}"):
            rs[p, 5].wait_recv()
            rs[p, 3].wait_recv()
            add_in(p, 1, 1, 5)
            rs[p, 1].start()

    gx_up, gx_down = (gx + 1) % 8, (gx + 7) % 8
    gy_up, gy_down = (gy + 1) % 8, (gy + 7) % 8

    def halo_copies(block, which):
        side = [
            ((gx, gy_up, gz), 0, slice(0, 8), slice(3, 11)),
            ((gx, gy_down, gz), 1, slice(0, 8), slice(3, 11)),
            ((gx_up, gy_up, gz), 0, slice(5, 8), slice(0, 3)),
            ((gx_up, gy_down, gz), 1, slice(5, 8), slice(0, 3)),
            ((gx_down, gy_up, gz), 0, slice(0, 3), slice(11, 14)),
            ((gx_down, gy_down, gz), 1, slice(0, 3), slice(11, 14)),
        ]
        end = [
            ((gx_up, gy, gz), slice(rows - HALO, rows), slice(0, 3)),
            ((gx_down, gy, gz), slice(0, HALO), slice(3, 6)),
        ]
        sem = [halo_sem.at[which * 3 + k] for k in range(3)]
        return [
            remote(faces.at[which, d, src], sides.at[which, d, dst], sem[0], sem[1], peer)
            for peer, d, src, dst in side
        ] + [
            remote(block.at[src], ends.at[which, dst], sem[0], sem[2], peer)
            for peer, src, dst in end
        ]

    def halo_waits(which):
        sem = [halo_sem.at[which * 3 + k] for k in range(3)]
        return (
            remote(sides.at[which], sides.at[which], sem[0], sem[1], along_y(1)),
            remote(ends.at[which], ends.at[which], sem[0], sem[2], along_y(1)),
        )

    with jax.named_scope("velocity_halo"):
        pl.semaphore_wait(met.at[2], 2)
        for copy in halo_copies(vel, 0):
            copy.start()

    for p in range(3):
        with jax.named_scope(f"hop2b#p={p}"):
            rs[p, 4].wait_recv()
            rs[p, 2].wait_recv()
            add_in(p, 0, 0, 4)
    square = jnp.zeros((8, 128), jnp.float32)
    for p, (r0, r1) in enumerate(STREAMS):
        with jax.named_scope(f"hop3#p={p}"):
            rs[p, 1].wait_recv()
            for n in range(r0, r1):
                value = w[0, n] + r[6, n]
                g_out[n] = value
                value = value * value
                square = square + (value[:8] + value[8:])
    ss[0] = square

    flat = [
        (((x + rx) % 4) * 2 + zl, gy, (gz + ry) % 4)
        for rx in range(4) for ry in range(4) if rx or ry
    ]
    tall = []
    for rz in range(8):
        for rc in range(2):
            if rz or rc:
                zz = (z + rz) % 8
                tall.append((x * 2 + zz % 2, (zz // 2) * 2 + (core + rc) % 2, gz))

    with jax.named_scope("send_squares"):
        for n, peer in enumerate(flat):
            remote(ss.at[0], a1.at[n], ar_sem.at[0], ar_sem.at[1], peer).start()
        fold_faces(g_out, 1)
        for copy in halo_copies(g_out, 1):
            copy.start()

    lane = lax.broadcasted_iota(jnp.int32, (24, 128), 1)

    def ring_row(block, which, n):
        inner = ends[which, n] if n < HALO else block[n - HALO] if n < rows + HALO else ends[which, n - rows]
        k = n if n < 11 else n - 8
        below, above = sides[which, 0, k], sides[which, 1, k]
        if n < HALO or 11 <= n < rows + HALO:
            beyond = pltpu.roll(jnp.where(low_half, below, above), 4, 0)
        else:
            beyond = jnp.where(low_half, above, below)
        return jnp.concatenate([inner, beyond], 0)

    def pack(block, which, ring):
        high = low = jnp.zeros((24, 128), jnp.float32)
        for n in range(wide):
            row = ring_row(block, which, n)
            ring[n] = row
            mine = (lane >= HIGH * n) & (lane < HIGH * (n + 1))
            high = jnp.where(mine, pltpu.roll(row, HIGH * n + 2, 1), high)
            if n:
                mine = (lane >= LOW * (n - 1)) & (lane < LOW * n)
                low = jnp.where(mine, pltpu.roll(row, (LOW * n + 125) % 128, 1), low)
        packs[2 * which] = high
        packs[2 * which + 1] = low
        for n, step in ((0, -1), (1, 1)):
            k = 2 * which + n
            remote(
                packs.at[k], landed.at[k], pack_sem.at[2 * which], pack_sem.at[2 * which + 1], along_y(step)
            ).start()

    def pack_wait(which):
        both = slice(2 * which, 2 * which + 2)
        return remote(
            packs.at[both], landed.at[both], pack_sem.at[2 * which], pack_sem.at[2 * which + 1], along_y(1)
        )

    squares1 = remote(a1, a1, ar_sem.at[0], ar_sem.at[1], along_y(1))
    squares2 = remote(a2, a2, ar_sem.at[2], ar_sem.at[3], along_y(1))
    with jax.named_scope("wait_squares1"):
        squares1.wait_recv()
        total = ss[0]
        for n in range(15):
            total = total + a1[n]
        ss[1] = total
        for n, peer in enumerate(tall):
            remote(ss.at[1], a2.at[n], ar_sem.at[2], ar_sem.at[3], peer).start()

    with jax.named_scope("wait_v_halo"):
        for copy in halo_waits(0):
            copy.wait_recv()
    with jax.named_scope("pack_v"):
        pack(vel, 0, t_out)
    with jax.named_scope("wait_g_halo"):
        for copy in halo_waits(1):
            copy.wait_recv()
    with jax.named_scope("pack_g"):
        pack(g_out, 1, ring_g)
    with jax.named_scope("wait_packs"):
        pack_wait(0).wait_recv()
        pack_wait(1).wait_recv()

    with jax.named_scope("wait_squares2"):
        squares2.wait_recv()
    with jax.named_scope("target"):
        total = ss[1]
        for n in range(15):
            total = total + a2[n]
        mean_square = jnp.sum(total, keepdims=True) * (1.0 / cells)
        scale = STEP_LENGTH * lax.rsqrt(mean_square + 1.0)
        for n in range(wide):
            t_out[n] = t_out[n] - scale * ring_g[n]
        for n, out in ((0, eh_out), (1, el_out)):
            out[0] = packs[n] - scale * packs[2 + n]
            out[1] = landed[n] - scale * landed[2 + n]

    with jax.named_scope("drain"):
        remote(r, r, rs_send.at[0], rs_recv.at[0], along_y(1)).wait_send()
        squares1.wait_send()
        squares2.wait_send()
        for which in range(2):
            for copy in halo_waits(which):
                copy.wait_send()
            pack_wait(which).wait_send()


def tv_kernel(sizes, t_in, eh_in, el_in, g_in, g_out, u_hbm, cur, bar, dx, dy, dz, u_out, out_sem):
    nx, ny, nz = sizes
    gx, gy, gz = lax.axis_index("gx"), lax.axis_index("gy"), lax.axis_index("gz")
    rows = g_in.shape[0]
    lanes = 128
    shape = (24, 128)
    lane = lax.broadcasted_iota(jnp.int32, shape, 1)
    ring = lax.broadcasted_iota(jnp.int32, shape, 0)

    def steps(position, count):
        inside = (position >= 0) & (position < count - 1)
        return jnp.where(inside, jnp.float32(DUAL_STEP), jnp.float32(0.0))

    step_y = steps(gy * 16 + jnp.where(ring < 20, ring, ring - 24), ny)
    step_z = steps(gz * lanes + lane, nz)
    step_x = [steps(gx * rows + n - HALO, nx) for n in range(rows + 2 * HALO)]

    g_copy = pltpu.make_async_copy(g_in, g_out, out_sem.at[0])
    g_copy.start()

    def shrink(a, b, c):
        norm = a * a + b * b + c * c
        limit = TV_WEIGHT * TV_WEIGHT
        return jnp.where(norm > limit, TV_WEIGHT * lax.rsqrt(norm), 1.0)

    def up(field, axis, by=1):
        return pltpu.roll(field, field.shape[axis] - by, axis)

    def down(field, axis, by=1):
        return pltpu.roll(field, by, axis)

    def primal(current, spread, target_part):
        return (current + PRIMAL_STEP * spread + target_part) * (1.0 / (1.0 + PRIMAL_STEP))

    class Edge:
        def __init__(self, own, other, width, first_row, first_plane, mine):
            plane = lane % width
            self.width = width
            self.target = jnp.where(mine(plane), own, other)
            self.tpart = PRIMAL_STEP * self.target
            self.current = self.bar = self.target
            self.step_x = steps(gx * rows + first_row + lane // width, nx)
            self.step_z = steps(gz * lanes + first_plane + plane, nz)
            self.dual = None

        def ascend(self):
            b = self.bar
            a = self.step_x * (up(b, 1, self.width) - b)
            c = step_y * (up(b, 0) - b)
            d = self.step_z * (up(b, 1) - b)
            if self.dual is not None:
                a, c, d = self.dual[0] + a, self.dual[1] + c, self.dual[2] + d
            f = shrink(a, c, d)
            self.dual = (a * f, c * f, d * f)

        def descend(self):
            a, c, d = self.dual
            spread = (a - down(a, 1, self.width)) + (c - down(c, 0)) + (d - down(d, 1))
            new = primal(self.current, spread, self.tpart)
            self.bar = 2.0 * new - self.current
            self.current = new

    high = Edge(eh_in[0], eh_in[1], HIGH, -HALO, lanes - 2, lambda k: k < 2)
    low = Edge(el_in[0], el_in[1], LOW, 1 - HALO, -3, lambda k: k >= 3)

    last = lane == lanes - 1
    head = lane == 0
    for it in range(ITERS):
        final = it == ITERS - 1
        source = t_in if it == 0 else bar
        present = t_in if it == 0 else cur
        above = high.bar
        low.ascend()
        below = low.dual[2]
        if not final:
            low.descend()
            high.ascend()
            high.descend()
        stop = rows + 2 * HALO - 1 - it
        previous_dx = None
        here = source[it]
        for n in range(it, stop):
            after = source[n + 1]
            beyond = pltpu.roll(above, (lanes - 1 - (HIGH * n + 2)) % lanes, 1)
            a = step_x[n] * (after - here)
            b = step_y * (up(here, 0) - here)
            c = step_z * (jnp.where(last, beyond, up(here, 1)) - here)
            if it:
                a, b, c = dx[n] + a, dy[n] + b, dz[n] + c
            f = shrink(a, b, c)
            a, b, c = a * f, b * f, c * f
            if not final:
                dx[n], dy[n], dz[n] = a, b, c
            if n > it:
                under = pltpu.roll(below, (lanes - (LOW * (n - 1) + 2)) % lanes, 1)
                spread = (a - previous_dx) + (b - down(b, 0)) + (c - jnp.where(head, under, down(c, 1)))
                now = present[n]
                new = primal(now, spread, PRIMAL_STEP * t_in[n])
                if final:
                    u_out[n - HALO] = new[:16]
                else:
                    bar[n] = 2.0 * new - now
                    cur[n] = new
            previous_dx = a
            here = after

    u_copy = pltpu.make_async_copy(u_out, u_hbm, out_sem.at[1])
    u_copy.start()
    g_copy.wait()
    u_copy.wait()


def shards(partials, code_bits, group_map, velocity):
    slots, nx, block_y, block_z = partials.shape
    block_x = velocity.shape[0]
    sizes = (
        block_x * lax.axis_size("gx"),
        block_y * lax.axis_size("gy"),
        block_z * lax.axis_size("gz"),
    )
    wide = block_x + 2 * HALO
    f32 = functools.partial(pltpu.VMEM, dtype=jnp.float32)
    dma = pltpu.SemaphoreType.DMA
    hbm = pl.BlockSpec(memory_space=pltpu.HBM)
    vmem = pl.BlockSpec(memory_space=pltpu.VMEM)
    packed = f32((2, 24, 128))
    block = f32(velocity.shape)
    result = pltpu.HBM(velocity.shape, jnp.float32)
    target, high, low, gradient = pl.pallas_call(
        functools.partial(comm_kernel, sizes[0] * sizes[1] * sizes[2]),
        out_shape=(
            f32((wide, 24, 128)), packed, packed, block,
        ),
        in_specs=[hbm] * 4,
        out_specs=(vmem,) * 4,
        scratch_shapes=[
            f32(partials.shape),
            f32((8, block_x, 16, 128)),
            f32((7, block_x, 16, 128)),
            block,
            f32((2, 2, 8, 8, 128)),
            f32((2, 2, 14, 8, 128)),
            f32((2, 6, 16, 128)),
            f32((4, 24, 128)),
            f32((4, 24, 128)),
            f32((wide, 24, 128)),
            f32((2, 8, 128)),
            f32((15, 8, 128)),
            f32((15, 8, 128)),
            pltpu.SMEM(code_bits.shape, jnp.int32),
            pltpu.SMEM(group_map.shape, jnp.int32),
            dma((12,)), dma((3,)), dma((1,)), dma((21,)), dma((4,)), dma((6,)), dma((4,)),
            pltpu.SemaphoreType.REGULAR((3,)),
        ],
        compiler_params=pltpu.CompilerParams(
            collective_id=0, has_side_effects=True, vmem_limit_bytes=48 * 1024 * 1024
        ),
        name="decode_exchange",
    )(*(pltpu.with_memory_space_constraint(a, pltpu.HBM) for a in (partials, code_bits, group_map, velocity)))
    field = f32((wide, 24, 128))
    return pl.pallas_call(
        functools.partial(tv_kernel, sizes),
        out_shape=(result, result),
        in_specs=[vmem] * 4,
        out_specs=(hbm, hbm),
        scratch_shapes=[field] * 5 + [block, dma((2,))],
        compiler_params=pltpu.CompilerParams(vmem_limit_bytes=32 * 1024 * 1024),
        name="tv_steps",
    )(*(pltpu.with_memory_space_constraint(a, pltpu.VMEM) for a in (target, high, low, gradient)))


def solution(mesh):
    split = P("gx", "gy", "gz")
    return jax.shard_map(
        shards,
        mesh=mesh,
        in_specs=(P("gx", None, "gy", "gz"), P(), P(), split),
        out_specs=(split, split),
        check_vma=False,
    )
```
